8 devices in a mesh: prompts: 1 (over z), model: 2 (over y), resp: 4 (over x, core).
Axes of the slice: x: 2, y: 2, z: 1, core: 2. Of those that a mesh axis runs over, the one named last changes fastest.
Arguments:
- x_prompt: bfloat16 [512, 1536], P(('prompts', 'resp'))
- x_resp: bfloat16 [4, 1024, 1536], P(('prompts', 'resp'))
- targets: int32 [4, 1024], P(('prompts', 'resp'))
- attn_norm: float32 [2, 1536], replicated
- mlp_norm: float32 [2, 1536], replicated
- w_q: bfloat16 [2, 1536, 12, 128], P(None, None, 'model')
- w_k: bfloat16 [2, 1536, 2, 128], P(None, None, 'model')
- w_v: bfloat16 [2, 1536, 2, 128], P(None, None, 'model')
- w_o: bfloat16 [2, 12, 128, 1536], P(None, 'model')
- w_gate: bfloat16 [2, 1536, 8960], P(None, None, 'model')
- w_up: bfloat16 [2, 1536, 8960], P(None, None, 'model')
- w_down: bfloat16 [2, 8960, 1536], P(None, 'model')
- final_norm: float32 [1536], replicated
- w_head: bfloat16 [1536, 8192], P(None, 'model')
Outputs:
- output: float32 [4, 1024], P(('prompts', 'resp'))
All inputs are finite; a program needn't handle non-finite values.
Results may differ from the reference program's by a relative error of at most 0.00308508.
Values are sent between devices in bfloat16 or wider.
A program may use at most 1 GiB of HBM per device.

```python
import math
import jax
import jax.numpy as jnp
from jax import lax

D_MODEL = 1536
N_HEADS = 12
KV_HEADS = 2
HEAD_DIM = 128
FF_DIM = 8960
PROMPT_DEV = 128
RESP_LEN = 1024
VOCAB_SLICE = 8192
GROUP_SIZE = 4
N_LAYERS = 2
ROPE_BASE = 10000
PROMPT_LEN = PROMPT_DEV * GROUP_SIZE
Q_GROUP = N_HEADS // KV_HEADS
RMS_EPS = 1e-6
NEG_BIG = -1e30


def setup_inputs(seed: int = 0, part: int = 0) -> dict:
    root_key = jax.random.key(seed)
    data_root, weight_root = jax.random.split(root_key)
    data_keys = jax.random.split(jax.random.fold_in(data_root, part), 5)
    weight_keys = jax.random.split(weight_root, 12)

    def normal_weight(rng_key, arr_shape, fan_in, w_gain):
        raw_draw = jax.random.normal(rng_key, arr_shape, jnp.float32)
        return (raw_draw * (w_gain / math.sqrt(fan_in))).astype(jnp.bfloat16)

    def norm_gains(rng_key, arr_shape):
        return jax.random.uniform(rng_key, arr_shape, jnp.float32, 0.5, 1.5)

    prompt_mean = jax.random.normal(data_keys[0], (1, D_MODEL), jnp.float32) * 0.7
    piece_shift = jax.random.normal(data_keys[1], (GROUP_SIZE, 1, D_MODEL), jnp.float32) * 0.7
    prompt_noise = jax.random.normal(data_keys[2], (GROUP_SIZE, PROMPT_DEV, D_MODEL), jnp.float32)
    x_prompt = (prompt_noise + piece_shift + prompt_mean).reshape(PROMPT_LEN, D_MODEL).astype(jnp.bfloat16)
    x_resp = jax.random.normal(data_keys[3], (GROUP_SIZE, RESP_LEN, D_MODEL), jnp.float32).astype(jnp.bfloat16)
    flat_ids = jax.random.randint(data_keys[4], (GROUP_SIZE * RESP_LEN,), 0, VOCAB_SLICE, dtype=jnp.int32)
    slot_ids = jnp.arange(GROUP_SIZE * RESP_LEN)
    flat_ids = jnp.where(slot_ids == 0, VOCAB_SLICE - 1, jnp.where(slot_ids == 1, 0, flat_ids))
    targets = flat_ids.reshape(GROUP_SIZE, RESP_LEN).astype(jnp.int32)
    return {
        'x_prompt': x_prompt,
        'x_resp': x_resp,
        'targets': targets,
        'attn_norm': norm_gains(weight_keys[0], (N_LAYERS, D_MODEL)),
        'mlp_norm': norm_gains(weight_keys[1], (N_LAYERS, D_MODEL)),
        'w_q': normal_weight(weight_keys[2], (N_LAYERS, D_MODEL, N_HEADS, HEAD_DIM), D_MODEL, 1.0),
        'w_k': normal_weight(weight_keys[3], (N_LAYERS, D_MODEL, KV_HEADS, HEAD_DIM), D_MODEL, 1.0),
        'w_v': normal_weight(weight_keys[4], (N_LAYERS, D_MODEL, KV_HEADS, HEAD_DIM), D_MODEL, 1.0),
        'w_o': normal_weight(weight_keys[5], (N_LAYERS, N_HEADS, HEAD_DIM, D_MODEL), N_HEADS * HEAD_DIM, 1.0),
        'w_gate': normal_weight(weight_keys[6], (N_LAYERS, D_MODEL, FF_DIM), D_MODEL, 1.0),
        'w_up': normal_weight(weight_keys[7], (N_LAYERS, D_MODEL, FF_DIM), D_MODEL, 1.0),
        'w_down': normal_weight(weight_keys[8], (N_LAYERS, FF_DIM, D_MODEL), FF_DIM, 1.0),
        'final_norm': norm_gains(weight_keys[9], (D_MODEL,)),
        'w_head': normal_weight(weight_keys[10], (D_MODEL, VOCAB_SLICE), D_MODEL, 3.0),
    }


def rms_norm(x_in, norm_gain):
    x_f = x_in.astype(jnp.float32)
    mean_sq = jnp.mean(x_f * x_f, axis=-1, keepdims=True)
    return (x_f * lax.rsqrt(mean_sq + RMS_EPS) * norm_gain).astype(jnp.bfloat16)


def rope_tables(positions):
    inv_freq = jnp.exp(jnp.arange(0, HEAD_DIM, 2, dtype=jnp.float32) * (-math.log(ROPE_BASE) / HEAD_DIM))
    angles = positions.astype(jnp.float32)[:, None] * inv_freq[None, :]
    return jnp.cos(angles), jnp.sin(angles)


def apply_rope(proj_f, cos_tab, sin_tab):
    half_dim = proj_f.shape[-1] // 2
    lo_half = proj_f[..., :half_dim]
    hi_half = proj_f[..., half_dim:]
    cos_b = cos_tab[:, None, :]
    sin_b = sin_tab[:, None, :]
    return jnp.concatenate([lo_half * cos_b - hi_half * sin_b, hi_half * cos_b + lo_half * sin_b], axis=-1)


def project_heads(hidden, w_mat):
    n_out = w_mat.shape[1] * w_mat.shape[2]
    proj_flat = jnp.dot(hidden, w_mat.reshape(D_MODEL, n_out), preferred_element_type=jnp.float32)
    return proj_flat.reshape(hidden.shape[0], w_mat.shape[1], HEAD_DIM)


def attend(queries, key_rows, val_rows, q_pos, k_pos):
    q_len = queries.shape[0]
    q_grp = queries.reshape(q_len, KV_HEADS, Q_GROUP, HEAD_DIM).astype(jnp.float32)
    scores = jnp.einsum('qhre,khe->hrqk', q_grp, key_rows.astype(jnp.float32)) * (1.0 / math.sqrt(HEAD_DIM))
    scores = jnp.where(k_pos[None, :] <= q_pos[:, None], scores, NEG_BIG)
    attn_probs = jax.nn.softmax(scores, axis=-1).astype(jnp.bfloat16).astype(jnp.float32)
    attn_mix = jnp.einsum('hrqk,khe->qhre', attn_probs, val_rows.astype(jnp.float32))
    return attn_mix.reshape(q_len, N_HEADS, HEAD_DIM).astype(jnp.bfloat16)


def finish_layer(x_in, attn_mix, w_out, gain_mlp, w_gate_l, w_up_l, w_down_l):
    attn_proj = jnp.dot(attn_mix.reshape(attn_mix.shape[0], N_HEADS * HEAD_DIM), w_out.reshape(N_HEADS * HEAD_DIM, D_MODEL), preferred_element_type=jnp.float32)
    x_mid = (x_in.astype(jnp.float32) + attn_proj).astype(jnp.bfloat16)
    hidden = rms_norm(x_mid, gain_mlp)
    gate_proj = jnp.dot(hidden, w_gate_l, preferred_element_type=jnp.float32)
    up_proj = jnp.dot(hidden, w_up_l, preferred_element_type=jnp.float32)
    act_vals = (jax.nn.silu(gate_proj) * up_proj).astype(jnp.bfloat16)
    down_proj = jnp.dot(act_vals, w_down_l, preferred_element_type=jnp.float32)
    return (x_mid.astype(jnp.float32) + down_proj).astype(jnp.bfloat16)


def reference(x_prompt, x_resp, targets, attn_norm, mlp_norm, w_q, w_k, w_v, w_o, w_gate, w_up, w_down, final_norm, w_head):
    prompt_pos = jnp.arange(PROMPT_LEN)
    resp_pos = PROMPT_LEN + jnp.arange(RESP_LEN)
    all_pos = jnp.concatenate([prompt_pos, resp_pos])
    p_cos, p_sin = rope_tables(prompt_pos)
    r_cos, r_sin = rope_tables(resp_pos)

    def kv_of(hidden, layer_idx, cos_tab, sin_tab):
        k_rot = apply_rope(project_heads(hidden, w_k[layer_idx]), cos_tab, sin_tab).astype(jnp.bfloat16)
        v_proj = project_heads(hidden, w_v[layer_idx]).astype(jnp.bfloat16)
        return k_rot, v_proj

    hidden_p = rms_norm(x_prompt, attn_norm[0])
    q_prompt = apply_rope(project_heads(hidden_p, w_q[0]), p_cos, p_sin).astype(jnp.bfloat16)
    k_one, v_one = kv_of(hidden_p, 0, p_cos, p_sin)

    def prompt_block(block_in):
        q_block, pos_block = block_in
        return attend(q_block, k_one, v_one, pos_block, prompt_pos)

    mix_prompt = lax.map(prompt_block, (q_prompt.reshape(GROUP_SIZE, PROMPT_DEV, N_HEADS, HEAD_DIM), prompt_pos.reshape(GROUP_SIZE, PROMPT_DEV)))
    x_prompt_one = finish_layer(x_prompt, mix_prompt.reshape(PROMPT_LEN, N_HEADS, HEAD_DIM), w_o[0], mlp_norm[0], w_gate[0], w_up[0], w_down[0])
    k_two, v_two = kv_of(rms_norm(x_prompt_one, attn_norm[1]), 1, p_cos, p_sin)
    prompt_cache = ((k_one, v_one), (k_two, v_two))

    def one_response(resp_in):
        x_cur, tgt_row = resp_in
        for layer_idx in range(N_LAYERS):
            k_cache, v_cache = prompt_cache[layer_idx]
            hidden = rms_norm(x_cur, attn_norm[layer_idx])
            q_resp = apply_rope(project_heads(hidden, w_q[layer_idx]), r_cos, r_sin).astype(jnp.bfloat16)
            k_resp, v_resp = kv_of(hidden, layer_idx, r_cos, r_sin)
            attn_mix = attend(q_resp, jnp.concatenate([k_cache, k_resp]), jnp.concatenate([v_cache, v_resp]), resp_pos, all_pos)
            x_cur = finish_layer(x_cur, attn_mix, w_o[layer_idx], mlp_norm[layer_idx], w_gate[layer_idx], w_up[layer_idx], w_down[layer_idx])
        logits = jnp.dot(rms_norm(x_cur, final_norm), w_head, preferred_element_type=jnp.float32)
        log_norm = jax.nn.logsumexp(logits, axis=-1)
        picked = jnp.sum(jnp.where(jnp.arange(VOCAB_SLICE)[None, :] == tgt_row[:, None], logits, 0.0), axis=-1)
        return picked - log_norm

    return lax.map(one_response, (x_resp, targets))
```

```python
import functools
import math
import jax
import jax.numpy as jnp
from jax import lax
from jax.experimental import pallas as pl
from jax.experimental.pallas import tpu as pltpu
from jax.sharding import PartitionSpec as P

RMS_EPS = 1e-6
ROPE_BASE = 10000.0
NEG_BIG = -1e30
LOG2E = 1.4426950408889634
CHUNKS = (2, 3, 3)
FF_BLOCK = 768
HEAD_BLOCK = 1024
ATTN_MIB, MLP_MIB, HEAD_MIB = 40, 60, 60
bf16, f32 = jnp.bfloat16, jnp.float32


def normed(x_in, gain):
    x_f = x_in.astype(f32)
    mean_sq = jnp.mean(x_f * x_f, axis=-1, keepdims=True)
    return (x_f * lax.rsqrt(mean_sq + RMS_EPS) * gain).astype(bf16)


def mm(a, b):
    return jnp.dot(a, b, preferred_element_type=f32)


def whole(shape):
    return pl.BlockSpec(shape, lambda *_: (0,) * len(shape), pipeline_mode=pl.Buffered(1))


ORDER_ONLY = pl.BlockSpec(memory_space=pl.ANY)


def call(body, name, flops, mib, grid, in_specs, out_shape, scratch, args, after):
    n_in, n_after = len(args), len(after)

    def run(*refs):
        body(*refs[:n_in], *refs[n_in + n_after:])

    return pl.pallas_call(
        run, name=name, grid=grid,
        in_specs=list(in_specs) + [ORDER_ONLY] * n_after,
        out_specs=[whole(o.shape) for o in out_shape], out_shape=out_shape, scratch_shapes=scratch,
        cost_estimate=pl.CostEstimate(flops=int(flops), bytes_accessed=0, transcendentals=0),
        compiler_params=pltpu.CompilerParams(vmem_limit_bytes=mib << 20),
    )(*args, *after)


def rotate(z, cos, sin):
    return (z * cos + pltpu.roll(z, z.shape[1] // 2, 1) * sin).astype(bf16)


def swapped(x, half):
    model = lax.axis_index('model')
    return x + jnp.where(x < half, (1 - model) * half, (model - 1) * half)


def causal(rows):
    q = swapped(lax.broadcasted_iota(jnp.int32, (rows, rows), 0), rows // 2)
    k = swapped(lax.broadcasted_iota(jnp.int32, (rows, rows), 1), rows // 2)
    return jnp.where(k <= q, 0.0, NEG_BIG)


def x_halves(xs, at, half):
    if at is None:
        model = lax.axis_index('model')
        pick = lambda side: [x[pl.ds(pl.multiple_of(side * (x.shape[0] // 2), 64), x.shape[0] // 2)] for x in xs]
        return [jnp.concatenate(p) if len(p) > 1 else p[0] for p in (pick(1 - model), pick(model))]
    return [x[at:at + half] for x in xs]


def load_h(h, xs, at, gain):
    half = h.shape[0] // 2
    lo, hi = x_halves(xs, at, half)
    h[:half] = normed(lo, gain[...])
    h[half:] = normed(hi, gain[...])


def rope_rows(steps, base, first, rows):
    half = rows // 2
    cos, sin = [], []
    for i in range(2):
        bc, bs = base[0, first + i:first + i + 1], base[1, first + i:first + i + 1]
        sc, ss = steps[0, :half], steps[1, :half]
        cos.append(bc * sc - bs * ss)
        sin.append(bs * sc + bc * ss)
    return jnp.concatenate(cos), jnp.concatenate(sin)


def layer_block(w, layer):
    return pl.BlockSpec((None,) + w.shape[1:], lambda *_: (layer,) + (0,) * (w.ndim - 1), pipeline_mode=pl.Buffered(1))


def rows_block(x, at, n):
    return pl.BlockSpec((pl.Element(n), pl.Element(x.shape[1])), lambda *_: (at, 0), pipeline_mode=pl.Buffered(1))


def prompt_body(at, first, *refs):
    *xs, gain, wq, wk, wv, steps, base, out, h = refs
    load_h(h, xs, at, gain)
    rows, dim = h.shape[0], wk.shape[1]
    cos, sin = rope_rows(steps, base, first, rows)
    n_q = out.shape[1] // dim - 2
    for i in range(0, n_q, 2):
        y = mm(h[...], jnp.concatenate([wq[i], wq[i + 1]], axis=1))
        out[:, i * dim:(i + 1) * dim] = rotate(y[:, :dim], cos, sin)
        out[:, (i + 1) * dim:(i + 2) * dim] = rotate(y[:, dim:], cos, sin)
    y = mm(h[...], jnp.concatenate([wk[...], wv[...]], axis=1))
    out[:, n_q * dim:(n_q + 1) * dim] = rotate(y[:, :dim], cos, sin)
    out[:, (n_q + 1) * dim:] = y[:, dim:].astype(bf16)


def prompt_qkv(xs, at, rows, gain, w, layer, steps, base, with_q, after=()):
    wq, wk, wv = w
    n_heads, d_model, dim = wq.shape[1:]
    cols = (n_heads + 2 if with_q else 2) * dim
    small = (gain, steps, base)
    return call(functools.partial(prompt_body, at, 0), 'prompt_qkv', 4 * rows * d_model * cols, 30, (1,),
                [whole(x.shape) for x in xs] + [whole(gain.shape)] + [layer_block(a, layer) for a in w] + [whole(steps.shape), whole(base.shape)],
                [jax.ShapeDtypeStruct((rows, cols), bf16)], [pltpu.VMEM((rows, d_model), bf16)],
                (*xs, gain, *w, steps, base), after)[0]


def attend(q, kbuf, vbuf, bias):
    dim, keys, masked = q.shape[1], kbuf.shape[0], bias.shape[1]
    free = keys - masked
    s = lax.dot_general(q, kbuf[...], (((1,), (1,)), ((), ())), preferred_element_type=f32)
    diag = jnp.where(bias[...] < 0, NEG_BIG, s[:, free:])
    s = jnp.concatenate([s[:, :free], diag], axis=1) if free else diag
    top = jnp.max(s, axis=-1, keepdims=True)
    e = jnp.exp2((s - top) * (LOG2E / math.sqrt(dim)))
    p = (e * (1.0 / jnp.sum(e, axis=-1, keepdims=True))).astype(bf16)
    return mm(p, vbuf[...]).astype(bf16)


def attn_body(n_x, at, first, n_kv, n_seen, prompt, *refs):
    refs = list(refs)
    take = lambda n: [refs.pop(0) for _ in range(n)]
    xs = take(n_x)
    gain, wq, wk, wv, steps, base = take(6)
    pieces, seen = take(n_kv), take(n_seen)
    qkv_p = take(1)[0] if prompt else None
    out, kv_new, h, kbuf, vbuf, bias = take(6)
    rows, dim = h.shape[0], wk.shape[1]
    half, n_q = rows // 2, wq.shape[0]
    load_h(h, xs, at, gain)
    cos, sin = rope_rows(steps, base, first, rows)
    bias[...] = causal(rows)
    fill = 0
    for r in pieces + seen:
        n = r.shape[0]
        kbuf[fill:fill + n] = r[:, :dim]
        vbuf[fill:fill + n] = r[:, dim:]
        fill += n
    y = mm(h[...], jnp.concatenate([wk[...], wv[...]], axis=1))
    k, v = rotate(y[:, :dim], cos, sin), y[:, dim:].astype(bf16)
    kv_new[:, :dim], kv_new[:, dim:] = k, v
    kbuf[fill:], vbuf[fill:] = k, v
    skip = 0
    if prompt:
        bias_p = take(1)[0]
        n_p, dev = qkv_p.shape[0], lax.axis_index('resp')
        skip = n_p // 2
        bias_p[:, :n_p] = causal(n_p)
        for s in range(1, n_kv):
            bias_p[:, s * n_p:(s + 1) * n_p] = jnp.full((n_p, n_p), jnp.where(dev >= s, 0.0, NEG_BIG), f32)
        for i in range(n_q):
            cols = slice(i * dim, (i + 1) * dim)
            mix = attend(qkv_p[:, cols], kbuf.at[:n_kv * n_p], vbuf.at[:n_kv * n_p], bias_p)
            out[:skip, cols] = mix[:skip]
            out[skip + half:2 * skip + half, cols] = mix[skip:]
    for i in range(0, n_q, 2):
        y = mm(h[...], jnp.concatenate([wq[i], wq[i + 1]], axis=1))
        for j in range(2):
            cols = slice((i + j) * dim, (i + j + 1) * dim)
            mix = attend(rotate(y[:, j * dim:(j + 1) * dim], cos, sin), kbuf, vbuf, bias)
            out[skip:skip + half, cols] = mix[:half]
            out[2 * skip + half:, cols] = mix[half:]


def attn_chunk(xs, x_specs, at, rows, gain, w, layer, steps, base, first, pieces, seen, qkv_p=None, after=()):
    wq, wk, wv = w
    n_heads, d_model, dim = wq.shape[1:]
    keys = sum(a.shape[0] for a in pieces + seen) + rows
    n_p = qkv_p.shape[0] if qkv_p is not None else 0
    extra = [qkv_p] if n_p else []
    out = [jax.ShapeDtypeStruct((rows + n_p, n_heads * dim), bf16), jax.ShapeDtypeStruct((rows, 2 * dim), bf16)]
    scratch = [pltpu.VMEM((rows, d_model), bf16), pltpu.VMEM((keys, dim), bf16), pltpu.VMEM((keys, dim), bf16), pltpu.VMEM((rows, rows), f32)]
    if n_p:
        scratch.append(pltpu.VMEM((n_p, n_p * len(pieces)), f32))
    rest = (*pieces, *seen, *extra)
    return call(functools.partial(attn_body, len(xs), at, first, len(pieces), len(seen), bool(n_p)), 'attn',
                2 * rows * d_model * n_heads * dim + 8 * rows * keys * n_heads * dim, ATTN_MIB, (1,),
                x_specs + [whole(gain.shape)] + [layer_block(a, layer) for a in w] + [whole(steps.shape), whole(base.shape)]
                + [whole(a.shape) for a in rest], out, scratch, (*xs, gain, *w, steps, base, *rest), after)


def mlp_body(n_x, at, ff, *refs):
    xs = refs[:n_x]
    a_own, a_far, wo_own, wo_far, gain, wg, wu, wd, send, keep, xm, g = refs[n_x:]
    step, blk, half = pl.program_id(0), wg.shape[1], send.shape[0]
    last = pl.num_programs(0) - 1
    rest = ff % blk or blk

    @pl.when(step == 0)
    def _():
        lo, hi = x_halves(xs, at, half)
        acc = mm(a_own[:half], wo_own[...]) + mm(a_far[half:], wo_far[...])
        g[:half] = normed((lo.astype(f32) + acc).astype(bf16), gain[...])
        acc = mm(a_own[half:], wo_own[...]) + mm(a_far[:half], wo_far[...])
        mid = (hi.astype(f32) + acc).astype(bf16)
        xm[...] = mid
        g[half:] = normed(mid, gain[...])

    def part(n):
        gate, up = mm(g[...], wg[:, :n]), mm(g[...], wu[:, :n])
        u = (gate * (1.0 / (1.0 + jnp.exp(-gate))) * up).astype(bf16)
        return mm(u, wd[:n])

    @pl.when(step == 0)
    def _():
        d = part(blk)
        send[...], keep[...] = d[:half], d[half:]

    @pl.when((step > 0) & (step < last))
    def _():
        d = part(blk)
        send[...] += d[:half]
        keep[...] += d[half:]

    @pl.when(step == last)
    def _():
        d = part(rest)
        send[...] += d[:half]
        keep[...] += d[half:]


def mlp_chunk(xs, x_specs, at, a_own, a_far, wo_own, wo_far, gain, wg, wu, wd, layer, after=()):
    rows, d_model, ff, blk = a_own.shape[0], xs[0].shape[1], wg.shape[2], FF_BLOCK
    half = rows // 2
    up_spec = pl.BlockSpec((None, d_model, blk), lambda j: (layer, 0, j))
    down_spec = pl.BlockSpec((None, blk, d_model), lambda j: (layer, j, 0))
    small = (a_own, a_far, wo_own, wo_far, gain)
    out = [jax.ShapeDtypeStruct((half, d_model), f32)] * 2 + [jax.ShapeDtypeStruct((half, d_model), bf16)]
    return call(functools.partial(mlp_body, len(xs), at, ff), 'mlp',
                6 * rows * d_model * ff + 4 * rows * d_model * wo_own.shape[0], MLP_MIB, (pl.cdiv(ff, blk),),
                x_specs + [whole(a.shape) for a in small] + [up_spec, up_spec, down_spec],
                out, [pltpu.VMEM((rows, d_model), bf16)], (*xs, *small, wg, wu, wd), after)


def head_body(row, xa, xb, gain, w, tgt, out, h, logits, top, pick):
    step, blk = pl.program_id(0), w.shape[1]

    @pl.when(step == 0)
    def _():
        load_h(h, (xa, xb), 0, gain)
        top[...] = jnp.full_like(top, NEG_BIG)
        pick[...] = jnp.zeros_like(pick)

    s = mm(h[...], w[...])
    logits[step] = s
    lanes = top.shape[1]
    hit = tgt[row:row + top.shape[0]] - step * blk
    lane = lax.broadcasted_iota(jnp.int32, top.shape, 1)
    best, found = top[...], pick[...]
    for c in range(0, blk, lanes):
        piece = s[:, c:c + lanes]
        best = jnp.maximum(best, piece)
        found += jnp.where(lane + c == hit, piece, 0.0)
    top[...], pick[...] = best, found

    @pl.when(step == pl.num_programs(0) - 1)
    def _():
        peak = jnp.max(top[...], axis=-1, keepdims=True)
        tot = jnp.zeros_like(top)
        for b in range(logits.shape[0]):
            for c in range(0, blk, lanes):
                tot += jnp.exp(logits[b, :, c:c + lanes] - peak)
        tot = jnp.sum(tot, axis=-1, keepdims=True)
        hits = jnp.sum(pick[...], axis=-1, keepdims=True)
        out[...] = jnp.where(lane == 0, peak, jnp.where(lane == 1, tot, hits))


def head_chunk(xa, xb, gain, w, tgt, row, after=()):
    d_model, vocab, blk = xa.shape[1], w.shape[1], HEAD_BLOCK
    rows = 2 * xa.shape[0]
    side = pltpu.VMEM((rows, 128), f32)
    return call(functools.partial(head_body, row), 'head', 4 * rows * d_model * vocab, HEAD_MIB, (vocab // blk,),
                [whole(xa.shape), whole(xb.shape), whole(gain.shape), pl.BlockSpec((d_model, blk), lambda j: (0, j)), whole(tgt.shape)],
                [jax.ShapeDtypeStruct((rows, 128), f32)],
                [pltpu.VMEM((rows, d_model), bf16), pltpu.VMEM((vocab // blk, rows, blk), f32), side, side],
                (xa, xb, gain, w, tgt), after)[0]


def rope_tables(positions, head_dim):
    inv_freq = jnp.exp(jnp.arange(0, head_dim, 2, dtype=f32) * (-math.log(ROPE_BASE) / head_dim))
    angles = positions.astype(f32)[:, None] * inv_freq[None, :]
    cos, sin = jnp.cos(angles), jnp.sin(angles)
    return jnp.stack([jnp.concatenate([cos, cos], axis=1), jnp.concatenate([-sin, sin], axis=1)])


def held(x, *after):
    return lax.optimization_barrier((x, *after))[0]


def solution(mesh):
    group = mesh.shape['resp']
    rows_spec = P(('prompts', 'resp'), None)
    in_specs = (rows_spec, P(('prompts', 'resp'), None, None), rows_spec, P(), P(),
                P(None, None, 'model', None), P(None, None, 'model', None), P(None, None, 'model', None),
                P(None, 'model', None, None), P(None, None, 'model'), P(None, None, 'model'),
                P(None, 'model', None), P(), P(None, 'model'))

    def across(x):
        return lax.ppermute(x, 'model', [(0, 1), (1, 0)])

    def all_pieces(x):
        return [x] + [lax.ppermute(x, 'resp', [(i, (i + s) % group) for i in range(group)]) for s in range(1, group)]

    def local_pass(x_piece, x_own, tgt_own, attn_norm, mlp_norm, w_q, w_k, w_v, w_o, w_gate, w_up, w_down, final_norm, w_head):
        n_layers, d_model, heads_loc, dim = w_q.shape
        piece_len, resp_len = x_piece.shape[0], x_own.shape[1]
        prompt_len = piece_len * group
        dev_idx, model_idx = lax.axis_index('resp'), lax.axis_index('model')
        sizes = [resp_len * n // sum(CHUNKS) for n in CHUNKS]
        starts = [sum(sizes[:c]) for c in range(len(sizes))]
        n_chunks = len(sizes)

        def sent_part(w):
            n = w.shape[0] // group
            return lax.dynamic_slice_in_dim(w, dev_idx * n, n, 0)

        def joined(part):
            return lax.all_gather(part, 'resp', axis=0, tiled=True)

        w_out = [w_o[l].reshape(heads_loc * dim, d_model) for l in range(n_layers)]
        w_heads = [[w_q[l].transpose(1, 0, 2)[None], w_k[l].reshape(1, d_model, dim), w_v[l].reshape(1, d_model, dim)]
                   for l in range(n_layers)]
        far_part = [across(sent_part(w)) for w in w_out]

        def halves(x, at, n):
            half = n // 2
            return (lax.dynamic_slice_in_dim(x, at + (1 - model_idx) * half, half, 0),
                    lax.dynamic_slice_in_dim(x, at + model_idx * half, half, 0))

        steps = rope_tables(jnp.arange(max(sizes) // 2), dim)
        both = jnp.stack([1 - model_idx, model_idx])
        base = rope_tables(jnp.concatenate([dev_idx * piece_len + both * (piece_len // 2)] + [
            prompt_len + at + both * (n // 2) for at, n in zip(starts, sizes)]), dim)
        tgt = jnp.concatenate([h for at, n in zip(starts, sizes) for h in halves(tgt_own[0] - model_idx * w_head.shape[1], at, n)])[:, None]
        x_rows = x_own[0]

        def source(l, c, with_prompt):
            n = sizes[c]
            if l == 0:
                xs = ([x_piece] if with_prompt else []) + [x_rows]
                return xs, ([whole(x_piece.shape)] if with_prompt else []) + [rows_block(x_rows, starts[c], n)], None
            return x_r[c], [whole(x.shape) for x in x_r[c]], piece_len // 2 if c == 0 else 0

        x_r = [None] * n_chunks
        pending = {}

        def mlp_of(l, c, a, wo_far, after):
            xs, specs, at = source(l, c, c == 0)
            send, keep, xm = mlp_chunk(xs, specs, at, *a, w_out[l], wo_far, mlp_norm[l][None], w_gate, w_up, w_down, l, after)
            pending[c] = (send, keep, xm)
            return keep

        def collect(c, far):
            _, keep, xm = pending.pop(c)
            mine = (xm.astype(f32) + (keep + far)).astype(bf16)
            x_r[c] = [across(mine), mine]
            return mine

        gain = attn_norm[0][None]
        qkv_p = prompt_qkv([x_piece], None, piece_len, gain, w_heads[0], 0, steps, base, True)
        pieces = all_pieces(qkv_p[:, heads_loc * dim:])
        wo_far = joined(held(far_part[0], qkv_p))
        w_heads[1] = [held(w, qkv_p) for w in w_heads[1]]
        a, seen, tail = [], [], ()
        for c in range(n_chunks):
            xs, specs, at = source(0, c, False)
            mix, kv = attn_chunk(xs, specs, at, sizes[c], gain, w_heads[0], 0, steps, base, 2 + 2 * c, pieces, list(seen),
                                 qkv_p if c == 0 else None, tail)
            seen.append(kv)
            a.append((mix, across(mix)))
            tail = (mix,)
        wo_far_next = joined(held(far_part[1], tail[0]))
        far = {}
        for c in range(n_chunks):
            tail = (mlp_of(0, c, a[c], wo_far, tail),)
            if c > 0:
                tail = (*tail, collect(c - 1, held(far[c - 1], *tail)))
            far[c] = across(held(pending[c][0], *tail))
        wo_far = wo_far_next

        gain = attn_norm[1][None]
        pieces = all_pieces(prompt_qkv(x_r[0], 0, piece_len, gain, w_heads[1], 0, steps, base, False, tail))
        a, seen = [], []
        done = 0
        for c in range(n_chunks):
            if c == n_chunks - 1:
                tail = (*tail, collect(c, far[c]))
            xs, specs, at = source(1, c, False)
            mix, kv = attn_chunk(xs, specs, at, sizes[c], gain, w_heads[1], 0, steps, base, 2 + 2 * c, pieces, list(seen), None, tail)
            seen.append(kv)
            a.append((mix, across(mix)))
            tail = (mix,)
            if c == n_chunks - 2:
                tail = (mlp_of(1, done, a[done], wo_far, tail),)
                far[done] = across(pending[done][0])
                done += 1
        while done < n_chunks:
            tail = (mlp_of(1, done, a[done], wo_far, tail),)
            tail = (*tail, collect(done - 1, held(far[done - 1], *tail)))
            far[done] = across(held(pending[done][0], *tail))
            done += 1
        stats = []
        for c in range(n_chunks):
            if c == n_chunks - 1:
                collect(c, held(far[c], *tail))
            stats.append(head_chunk(*x_r[c], final_norm[None], w_head, tgt, starts[c], tail))
            tail = (stats[-1],)
        here = jnp.concatenate([h for s, n in zip(stats, sizes) for h in halves(s[:, :3], 0, n)]).T
        there = across(here)
        top = jnp.maximum(here[0], there[0])
        tot = here[1] * jnp.exp(here[0] - top) + there[1] * jnp.exp(there[0] - top)
        logp = here[2] + there[2] - top - jnp.log(tot)
        return logp[None, :]

    return jax.shard_map(local_pass, mesh=mesh, in_specs=in_specs, out_specs=rows_spec, check_vma=False)
```

```python
import functools
import math
import jax
import jax.numpy as jnp
from jax import lax
from jax.experimental import pallas as pl
from jax.experimental.pallas import tpu as pltpu
from jax.sharding import PartitionSpec as P

RMS_EPS = 1e-6
ROPE_BASE = 10000.0
NEG_BIG = -1e30
LOG2E = 1.4426950408889634
CHUNKS = (2, 3, 3)
FF_BLOCK = 768
HEAD_BLOCK = 1024
KERNEL_MIB = 63
bf16, f32 = jnp.bfloat16, jnp.float32


def normed(x_in, gain):
    x_f = x_in.astype(f32)
    mean_sq = jnp.mean(x_f * x_f, axis=-1, keepdims=True)
    return (x_f * lax.rsqrt(mean_sq + RMS_EPS) * gain).astype(bf16)


def mm(a, b):
    return jnp.dot(a, b, preferred_element_type=f32)


def whole(shape):
    return pl.BlockSpec(shape, lambda *_: (0,) * len(shape), pipeline_mode=pl.Buffered(1))


ORDER_ONLY = pl.BlockSpec(memory_space=pl.ANY)


def call(body, flops, mib, grid, in_specs, out_shape, scratch, args, after):
    n_in, n_after = len(args), len(after)

    def run(*refs):
        body(*refs[:n_in], *refs[n_in + n_after:])

    return pl.pallas_call(
        run, grid=grid,
        in_specs=list(in_specs) + [ORDER_ONLY] * n_after,
        out_specs=[whole(o.shape) for o in out_shape], out_shape=out_shape, scratch_shapes=scratch,
        cost_estimate=pl.CostEstimate(flops=int(flops), bytes_accessed=0, transcendentals=0),
        compiler_params=pltpu.CompilerParams(vmem_limit_bytes=mib << 20),
    )(*args, *after)


def rotate(z, cos, sin):
    return (z * cos + pltpu.roll(z, z.shape[1] // 2, 1) * sin).astype(bf16)


def natural(i, rows):
    half, model = rows // 2, lax.axis_index('model')
    away = (1 - model) * half
    return i + jnp.where(i < half, away, -away)


def causal(rows):
    q = natural(lax.broadcasted_iota(jnp.int32, (rows, 1), 0), rows)
    k = natural(lax.broadcasted_iota(jnp.int32, (1, rows), 1), rows)
    return jnp.where(k <= q, 0.0, NEG_BIG)


def x_halves(xs, at, half):
    if at is not None:
        return [x[at:at + half] for x in xs]
    model = lax.axis_index('model')
    pick = lambda side: [x[pl.ds(pl.multiple_of(side * (x.shape[0] // 2), 64), x.shape[0] // 2)] for x in xs]
    return [jnp.concatenate(pick(side)) for side in (1 - model, model)]


def load_h(h, xs, at, gain):
    half = h.shape[0] // 2
    lo, hi = x_halves(xs, at, half)
    h[:half] = normed(lo, gain[...])
    h[half:] = normed(hi, gain[...])


def rope_rows(steps, base, first, rows):
    cos, sin = [], []
    sc, ss = steps[0, :rows // 2], steps[1, :rows // 2]
    for j in (first, first + 1):
        bc, bs = base[0, j:j + 1], base[1, j:j + 1]
        cos.append(bc * sc - bs * ss)
        sin.append(bs * sc + bc * ss)
    return jnp.concatenate(cos), jnp.concatenate(sin)


def layer_block(w, layer):
    return pl.BlockSpec((None,) + w.shape[1:], lambda *_: (layer,) + (0,) * (w.ndim - 1), pipeline_mode=pl.Buffered(1))


def rows_block(x, at, n):
    return pl.BlockSpec((pl.Element(n), pl.Element(x.shape[1])), lambda *_: (at, 0), pipeline_mode=pl.Buffered(1))


def prompt_body(parts, n_w, *refs):
    *xs, gain, steps, base = refs[:-3 * n_w - 2]
    ws, out, h = refs[-3 * n_w - 2:-2], refs[-2], refs[-1]
    load_h(h, xs, parts, gain)
    dim = ws[1].shape[1]
    cos, sin = rope_rows(steps, base, 0, h.shape[0])
    n_q = out.shape[1] // dim - 2 * n_w
    for i in range(0, n_q, 2):
        y = mm(h[...], jnp.concatenate([ws[0][i], ws[0][i + 1]], axis=1))
        out[:, i * dim:(i + 1) * dim] = rotate(y[:, :dim], cos, sin)
        out[:, (i + 1) * dim:(i + 2) * dim] = rotate(y[:, dim:], cos, sin)
    for i in range(n_w):
        y = mm(h[...], jnp.concatenate([ws[3 * i + 1][...], ws[3 * i + 2][...]], axis=1))
        c = (n_q + 2 * i) * dim
        out[:, c:c + dim] = rotate(y[:, :dim], cos, sin)
        out[:, c + dim:c + 2 * dim] = y[:, dim:].astype(bf16)


def prompt_qkv(xs, parts, rows, gain, ws, steps, base, with_q, after=()):
    n_heads, d_model, dim = ws[0][0][0].shape[1:]
    cols = (n_heads + 2 if with_q else 2 * len(ws)) * dim
    flat = [a for w in ws for a in w[0]]
    return call(functools.partial(prompt_body, parts, len(ws)), 4 * rows * d_model * cols, KERNEL_MIB, (1,),
                [whole(x.shape) for x in xs] + [whole(gain.shape), whole(steps.shape), whole(base.shape)] + [b for w in ws for b in w[1]],
                [jax.ShapeDtypeStruct((rows, cols), bf16)], [pltpu.VMEM((rows, d_model), bf16)],
                (*xs, gain, steps, base, *flat), after)[0]


def attend(q, kbuf, vbuf, bias):
    dim, keys, masked = q.shape[1], kbuf.shape[0], bias.shape[1]
    free = keys - masked
    s = lax.dot_general(q, kbuf[...], (((1,), (1,)), ((), ())), preferred_element_type=f32)
    diag = jnp.where(bias[...] < 0, NEG_BIG, s[:, free:])
    s = jnp.concatenate([s[:, :free], diag], axis=1) if free else diag
    top = jnp.max(s, axis=-1, keepdims=True)
    e = jnp.exp2((s - top) * (LOG2E / math.sqrt(dim)))
    p = (e * (1.0 / jnp.sum(e, axis=-1, keepdims=True))).astype(bf16)
    return mm(p, vbuf[...]).astype(bf16)


def attn_parts(n_x, n_w, parts, first, n_kv, n_seen, prompt, *refs):
    refs = list(refs)
    take = lambda n: [refs.pop(0) for _ in range(n)]
    xs = take(n_x)
    gain, steps, base = take(3)
    ws = [take(3) for _ in range(n_w)]
    pieces, seen = take(n_kv), take(n_seen)
    qkv_p = take(1)[0] if prompt else None
    out, kv_new, h, kbuf, vbuf, bias = take(6)
    bias_p = take(1)[0] if prompt else None
    rows, dim = h.shape[0], kbuf.shape[2]
    half, n_q = rows // 2, out.shape[1] // dim // n_w
    skip = qkv_p.shape[0] // 2 if prompt else 0

    def prepare():
        load_h(h, xs, parts, gain)
        bias[...] = causal(rows)
        if prompt:
            n_p, dev = qkv_p.shape[0], lax.axis_index('resp')
            bias_p[:, :n_p] = causal(n_p)
            for s in range(1, n_kv):
                bias_p[:, s * n_p:(s + 1) * n_p] = jnp.full((n_p, n_p), jnp.where(dev >= s, 0.0, NEG_BIG), f32)

    def side(m):
        wq, wk, wv = ws[m]
        cos, sin = rope_rows(steps, base, first, rows)
        fill, c = 0, 2 * m * dim
        for r in pieces + seen:
            n = r.shape[0]
            kbuf[m, fill:fill + n] = r[:, c:c + dim]
            vbuf[m, fill:fill + n] = r[:, c + dim:c + 2 * dim]
            fill += n
        y = mm(h[...], jnp.concatenate([wk[...], wv[...]], axis=1))
        k, v = rotate(y[:, :dim], cos, sin), y[:, dim:].astype(bf16)
        kv_new[:, c:c + dim], kv_new[:, c + dim:c + 2 * dim] = k, v
        kbuf[m, fill:], vbuf[m, fill:] = k, v
        if prompt:
            n_p = qkv_p.shape[0]
            for i in range(n_q):
                cols = slice(i * dim, (i + 1) * dim)
                mix = attend(qkv_p[:, cols], kbuf.at[m, :n_kv * n_p], vbuf.at[m, :n_kv * n_p], bias_p)
                out[:skip, cols] = mix[:skip]
                out[skip + half:2 * skip + half, cols] = mix[skip:]
        for i in range(0, n_q, 2):
            y = mm(h[...], jnp.concatenate([wq[i], wq[i + 1]], axis=1))
            for j in range(2):
                cols = slice((m * n_q + i + j) * dim, (m * n_q + i + j + 1) * dim)
                mix = attend(rotate(y[:, j * dim:(j + 1) * dim], cos, sin), kbuf.at[m], vbuf.at[m], bias)
                out[skip:skip + half, cols] = mix[:half]
                out[2 * skip + half:, cols] = mix[half:]

    def start():
        prepare()
        side(0)

    return [start] + [functools.partial(side, m) for m in range(1, n_w)]


def attn_body(*args):
    for part in attn_parts(*args):
        part()


def attn_chunk(xs, x_specs, parts, rows, gain, ws, steps, base, first, pieces, seen, qkv_p=None, after=()):
    d_model, dim = xs[0].shape[1], steps.shape[2]
    n_w, n_heads = len(ws), ws[0][2]
    keys = sum(a.shape[0] for a in pieces + seen) + rows
    n_p = qkv_p.shape[0] if qkv_p is not None else 0
    extra = [qkv_p] if n_p else []
    out = [jax.ShapeDtypeStruct((rows + n_p, n_w * n_heads * dim), bf16), jax.ShapeDtypeStruct((rows, 2 * n_w * dim), bf16)]
    buf = pltpu.VMEM((n_w, keys, dim), bf16)
    scratch = [pltpu.VMEM((rows, d_model), bf16), buf, buf, pltpu.VMEM((rows, rows), f32)]
    if n_p:
        scratch.append(pltpu.VMEM((n_p, n_p * len(pieces)), f32))
    rest = (*pieces, *seen, *extra)
    return call(functools.partial(attn_body, len(xs), n_w, parts, first, len(pieces), len(seen), bool(n_p)),
                n_w * (2 * rows * d_model * n_heads * dim + 8 * rows * keys * n_heads * dim), KERNEL_MIB, (1,),
                x_specs + [whole(gain.shape), whole(steps.shape), whole(base.shape)] + [b for w in ws for b in w[1]]
                + [whole(a.shape) for a in rest], out, scratch, (*xs, gain, steps, base, *[a for w in ws for a in w[0]], *rest), after)


def ffn_body(n_x, parts, layer, ff, attn, n_attn, *refs):
    refs = list(refs)
    take = lambda n: [refs.pop(0) for _ in range(n)]
    xs, gain, (wo_own, wo_far, wg, wu, wd), inputs = take(n_x), take(1)[0], take(5), take(n_attn)
    send, keep, xm = take(3)
    kv_new = take(1) if attn else []
    g, bo, bg, bu, bd, sems, *spare = refs
    step, blk, half = pl.program_id(0), bg.shape[2], send.shape[0]
    n_blk = pl.cdiv(ff, blk)
    rest = ff - (n_blk - 1) * blk
    n_pre = 1 + (attn[0] if attn else 0)

    def block_copies(j, slot, n):
        at = pl.multiple_of(j * blk, 128)
        return [pltpu.make_async_copy(wg.at[layer, :, pl.ds(at, n)], bg.at[slot, :, :n], sems.at[2 + 3 * slot]),
                pltpu.make_async_copy(wu.at[layer, :, pl.ds(at, n)], bu.at[slot, :, :n], sems.at[3 + 3 * slot]),
                pltpu.make_async_copy(wd.at[layer, pl.ds(at, n)], bd.at[slot, :n], sems.at[4 + 3 * slot])]

    @pl.when(step == 0)
    def _():
        wo_copies = [pltpu.make_async_copy(wo_own.at[layer], bo.at[0], sems.at[0]), pltpu.make_async_copy(wo_far, bo.at[1], sems.at[1])]
        for copy in wo_copies + block_copies(0, 0, blk):
            copy.start()

    if attn:
        mix, *buffers = spare
        for at, piece in enumerate(attn_parts(n_x, *attn, *xs, *inputs, mix, *kv_new, g, *buffers)):
            pl.when(step == at)(piece)

    @pl.when(step == n_pre - 1)
    def _():
        if attn:
            own, far = mix[:, :bo.shape[1]], mix[:, bo.shape[1]:]
        elif n_attn > 1:
            own, far = inputs[0][...], jnp.concatenate([inputs[1][half:], inputs[1][:half]])
        else:
            own, far = inputs[0][:, :bo.shape[1]], inputs[0][:, bo.shape[1]:]
        lo, hi = x_halves(xs, parts, half)
        wo_copies = [pltpu.make_async_copy(wo_own.at[layer], bo.at[0], sems.at[0]), pltpu.make_async_copy(wo_far, bo.at[1], sems.at[1])]
        wo_copies[0].wait()
        acc = mm(own, bo[0])
        wo_copies[1].wait()
        acc += mm(far, bo[1])
        g[:half] = normed((lo.astype(f32) + acc[:half]).astype(bf16), gain[...])
        mid = (hi.astype(f32) + acc[half:]).astype(bf16)
        xm[...] = mid
        g[half:] = normed(mid, gain[...])
        send[...] = jnp.zeros_like(send)
        keep[...] = jnp.zeros_like(keep)

    def part(slot, n):
        gate, up = mm(g[...], bg[slot, :, :n]), mm(g[...], bu[slot, :, :n])
        u = (gate * (1.0 / (1.0 + jnp.exp(-gate))) * up).astype(bf16)
        d = mm(u, bd[slot, :n])
        send[...] += d[:half]
        keep[...] += d[half:]

    j = step - n_pre
    slot = lax.rem(step + n_pre, 2)

    @pl.when((j >= 0) & (j + 1 < n_blk - 1))
    def _():
        for copy in block_copies(j + 1, 1 - slot, blk):
            copy.start()

    @pl.when(j + 1 == n_blk - 1)
    def _():
        for copy in block_copies(n_blk - 1, (n_blk - 1) % 2, rest):
            copy.start()

    @pl.when((j >= 0) & (j < n_blk - 1))
    def _():
        for copy in block_copies(j, slot, blk):
            copy.wait()
        part(slot, blk)

    @pl.when(j == n_blk - 1)
    def _():
        for copy in block_copies(n_blk - 1, (n_blk - 1) % 2, rest):
            copy.wait()
        part((n_blk - 1) % 2, rest)


def ffn_chunk(xs, x_specs, parts, layer, gain, wo_own, wo_far, wg, wu, wd, mix=None, attn=None, after=()):
    d_model, ff, blk = xs[0].shape[1], wg.shape[2], FF_BLOCK
    width = wo_far.shape[0]
    big = [pl.BlockSpec(memory_space=pl.ANY)] * 5
    flops = 6
    if attn is None:
        rows, inputs, in_specs, attn_static, spare, more = mix[0].shape[0], list(mix), [whole(a.shape) for a in mix], None, [], []
    else:
        rows, gain_a, ws, steps, base, first, pieces, seen = attn
        dim = steps.shape[2]
        keys = sum(a.shape[0] for a in pieces + seen) + rows
        inputs = [gain_a, steps, base, *[a for w in ws for a in w[0]], *pieces, *seen]
        in_specs = [whole(a.shape) for a in (gain_a, steps, base)] + [b for w in ws for b in w[1]] + [whole(a.shape) for a in pieces + seen]
        attn_static = (len(ws), parts, first, len(pieces), len(seen), False)
        buf = pltpu.VMEM((len(ws), keys, dim), bf16)
        spare = [pltpu.VMEM((rows, len(ws) * width), bf16), buf, buf, pltpu.VMEM((rows, rows), f32)]
        more = [jax.ShapeDtypeStruct((rows, 2 * len(ws) * dim), bf16)]
        flops = 8
    half = rows // 2
    out = [jax.ShapeDtypeStruct((half, d_model), f32)] * 2 + [jax.ShapeDtypeStruct((half, d_model), bf16)] + more
    scratch = [pltpu.VMEM((rows, d_model), bf16), pltpu.VMEM((2, width, d_model), bf16), pltpu.VMEM((2, d_model, blk), bf16),
               pltpu.VMEM((2, d_model, blk), bf16), pltpu.VMEM((2, blk, d_model), bf16), pltpu.SemaphoreType.DMA((8,))] + spare
    return call(functools.partial(ffn_body, len(xs), parts, layer, ff, attn_static, len(inputs)),
                flops * rows * d_model * ff, KERNEL_MIB, (1 + (attn_static[0] if attn else 0) + pl.cdiv(ff, blk),),
                x_specs + [whole(gain.shape)] + big + in_specs, out, scratch,
                (*xs, gain, wo_own, wo_far, wg, wu, wd, *inputs), after)


def head_body(row, xa, xb, gain, w, tgt, out, h, logits, top, pick):
    step, blk = pl.program_id(0), w.shape[1]

    @pl.when(step == 0)
    def _():
        load_h(h, (xa, xb), 0, gain)
        top[...] = jnp.full_like(top, NEG_BIG)
        pick[...] = jnp.zeros_like(pick)

    s = mm(h[...], w[...])
    logits[step] = s
    lanes = top.shape[1]
    hit = tgt[row:row + top.shape[0]] - step * blk
    lane = lax.broadcasted_iota(jnp.int32, top.shape, 1)
    best, found = top[...], pick[...]
    for c in range(0, blk, lanes):
        piece = s[:, c:c + lanes]
        best = jnp.maximum(best, piece)
        found += jnp.where(lane + c == hit, piece, 0.0)
    top[...], pick[...] = best, found

    @pl.when(step == pl.num_programs(0) - 1)
    def _():
        peak = jnp.max(top[...], axis=-1, keepdims=True)
        tot = jnp.zeros_like(top)
        for b in range(logits.shape[0]):
            for c in range(0, blk, lanes):
                tot += jnp.exp(logits[b, :, c:c + lanes] - peak)
        tot = jnp.sum(tot, axis=-1, keepdims=True)
        hits = jnp.sum(pick[...], axis=-1, keepdims=True)
        out[...] = jnp.where(lane == 0, peak, jnp.where(lane == 1, tot, hits))


def head_chunk(xa, xb, gain, w, tgt, row, after=()):
    d_model, vocab, blk = xa.shape[1], w.shape[1], HEAD_BLOCK
    rows = 2 * xa.shape[0]
    side = pltpu.VMEM((rows, 128), f32)
    return call(functools.partial(head_body, row), 4 * rows * d_model * vocab, KERNEL_MIB, (vocab // blk,),
                [whole(xa.shape), whole(xb.shape), whole(gain.shape), pl.BlockSpec((d_model, blk), lambda j: (0, j)), whole(tgt.shape)],
                [jax.ShapeDtypeStruct((rows, 128), f32)],
                [pltpu.VMEM((rows, d_model), bf16), pltpu.VMEM((vocab // blk, rows, blk), f32), side, side],
                (xa, xb, gain, w, tgt), after)[0]


def rope_tables(positions, head_dim):
    inv_freq = jnp.exp(jnp.arange(0, head_dim, 2, dtype=f32) * (-math.log(ROPE_BASE) / head_dim))
    angles = positions.astype(f32)[:, None] * inv_freq[None, :]
    cos, sin = jnp.cos(angles), jnp.sin(angles)
    return jnp.stack([jnp.concatenate([cos, cos], axis=1), jnp.concatenate([-sin, sin], axis=1)])


def held(x, *after):
    return lax.optimization_barrier((x, *after))[0]


def solution(mesh):
    group = mesh.shape['resp']
    rows_spec = P(('prompts', 'resp'), None)
    in_specs = (rows_spec, P(('prompts', 'resp'), None, None), rows_spec, P(), P(),
                P(None, None, 'model', None), P(None, None, 'model', None), P(None, None, 'model', None),
                P(None, 'model', None, None), P(None, None, 'model'), P(None, None, 'model'),
                P(None, 'model', None), P(), P(None, 'model'))

    def across(x):
        return lax.ppermute(x, 'model', [(0, 1), (1, 0)])

    def all_pieces(x):
        return [x] + [lax.ppermute(x, 'resp', [(i, (i + s) % group) for i in range(group)]) for s in range(1, group)]

    def local_pass(x_piece, x_own, tgt_own, attn_norm, mlp_norm, w_q, w_k, w_v, w_o, w_gate, w_up, w_down, final_norm, w_head):
        n_layers, d_model, heads_loc, dim = w_q.shape
        piece_len, resp_len = x_piece.shape[0], x_own.shape[1]
        prompt_len = piece_len * group
        dev_idx, model_idx = lax.axis_index('resp'), lax.axis_index('model')
        sizes = [resp_len * n // sum(CHUNKS) for n in CHUNKS]
        starts = [sum(sizes[:c]) for c in range(len(sizes))]
        n_chunks = len(sizes)

        def joined(part):
            return lax.all_gather(part, 'resp', axis=0, tiled=True)

        w_out = w_o.reshape(n_layers, heads_loc * dim, d_model)
        part = heads_loc * dim // group

        def wo_part(l, *after):
            x = lax.dynamic_slice(w_out, (l, dev_idx * part, 0), (1, part, d_model))[0]
            return across(held(x, *after))

        def own_heads(l, *after):
            w = (held(w_q, *after)[l].transpose(1, 0, 2)[None], w_k[l].reshape(1, d_model, dim), w_v[l].reshape(1, d_model, dim))
            return w, [layer_block(a, 0) for a in w], heads_loc

        def far_heads(w):
            spec = lambda n, i: pl.BlockSpec((n, d_model, dim), lambda *_: (i, 0, 0), pipeline_mode=pl.Buffered(1))
            return (w, w, w), [spec(heads_loc, 0), spec(None, heads_loc), spec(None, heads_loc + 1)], heads_loc

        def halves(x, at, n):
            half = n // 2
            return (lax.dynamic_slice_in_dim(x, at + (1 - model_idx) * half, half, 0),
                    lax.dynamic_slice_in_dim(x, at + model_idx * half, half, 0))

        steps = rope_tables(jnp.arange(max(sizes) // 2), dim)
        both = jnp.stack([1 - model_idx, model_idx])
        base = rope_tables(jnp.concatenate([dev_idx * piece_len + both * (piece_len // 2)] + [
            prompt_len + at + both * (n // 2) for at, n in zip(starts, sizes)]), dim)
        x_rows = x_own[0]

        def source(l, c, with_prompt):
            if l == 0:
                xs = ([x_piece] if with_prompt else []) + [x_rows]
                return xs, ([whole(x_piece.shape)] if with_prompt else []) + [rows_block(x_rows, starts[c], sizes[c])], None
            return x_r[c], [whole(x.shape) for x in x_r[c]], 0 if c else piece_len // 2

        x_r, far = {}, {}
        pending = {}

        def mlp_of(l, c, wo_far, after, mix=None, attn=None):
            xs, specs, parts = source(l, c, c == 0)
            *pending[c], = ffn_chunk(xs, specs, parts, l, mlp_norm[l][None], w_out, wo_far, w_gate, w_up, w_down, mix, attn, after)
            return pending[c][1]

        def send(c, *after):
            far[c] = across(held(pending[c][0], *after))

        def collect(c, *after):
            _, keep, xm = pending.pop(c)[:3]
            mine = (xm.astype(f32) + (keep + held(far.pop(c), *after))).astype(bf16)
            x_r[c] = [across(mine), mine]
            return mine

        end = n_chunks - 1
        gain = attn_norm[0][None]
        w_own = own_heads(0)
        qkv_p = prompt_qkv([x_piece], None, piece_len, gain, [w_own], steps, base, True)
        pieces = all_pieces(qkv_p[:, heads_loc * dim:])
        wo_sent = [wo_part(0, qkv_p)]
        w_next = own_heads(1, qkv_p)
        heads = jnp.concatenate([w_next[0][0][0], w_next[0][1], w_next[0][2]])
        per = heads.shape[0] // group
        w_part = across(lax.dynamic_slice_in_dim(heads, dev_idx * per, per, 0))
        a, seen, tail = [], [], ()
        for c in range(n_chunks):
            xs, specs, parts = source(0, c, False)
            mix, kv = attn_chunk(xs, specs, parts, sizes[c], gain, [w_own], steps, base, 2 + 2 * c, pieces, list(seen),
                                 qkv_p if c == 0 else None, tail)
            seen.append(kv)
            a.append((mix, across(mix)))
            tail = (mix,)
            if c == 0:
                wo_far = [joined(held(wo_sent[0], mix))]
        wo_sent.append(wo_part(1, a[-1][0]))
        for c in range(n_chunks):
            tail = (mlp_of(0, c, wo_far[0], tail, mix=a[c]),)
            if c == 0:
                w_far = far_heads(joined(held(w_part, *tail)))
                send(c)
            elif c < end or c == 1:
                tail = (*tail, collect(c - 1, *tail))
                if c < end:
                    send(c)
            if c == 1:
                wo_far.append(joined(held(wo_sent[1], *tail)))
        gain = attn_norm[1][None]
        both_w = [w_next, w_far]
        kv_p = prompt_qkv(x_r[0], 0, piece_len, gain, both_w, steps, base, False, tail)
        pieces = all_pieces(kv_p)
        tail = (kv_p, collect(end - 1, kv_p)) if end > 1 else (kv_p,)
        send(end)
        seen = []
        tail = (mlp_of(1, 0, wo_far[1], tail, attn=(sizes[0], gain, both_w, steps, base, 2, pieces, [])),)
        seen.append(pending[0][3])
        tail = (*tail, collect(end, *tail))
        send(0)

        def attention(c, ws, after):
            xs, specs, parts = source(1, c, False)
            mix, kv = attn_chunk(xs, specs, parts, sizes[c], gain, ws, steps, base, 2 + 2 * c, pieces, list(seen), None, after)
            seen.append(kv)
            return mix

        mixes = {}
        for c in range(1, n_chunks):
            mix = attention(c, both_w if c < end else both_w[:1], tail)
            mixes[c] = [mix] if c < end else [mix, across(mix)]
            tail = (mix,)
        for c in range(1, n_chunks):
            if c < end:
                tail = (*tail, collect(c - 1, *tail))
            tail = (mlp_of(1, c, wo_far[1], tail, mix=mixes[c]),)
            if c == end:
                collect(c - 1, *tail)
            send(c)
        tgt = tgt_own[0] - model_idx * w_head.shape[1]
        tgt = held(jnp.concatenate([h for at, n in zip(starts, sizes) for h in halves(tgt, at, n)]), *tail)[:, None]
        stats = []
        for c in range(n_chunks):
            if c == end:
                collect(c, *tail)
            out = head_chunk(*x_r[c], final_norm[None], w_head, tgt, starts[c], tail)
            tail = (out,)
            stats.append(jnp.concatenate(halves(out[:, :3], 0, sizes[c])))
        here = jnp.concatenate(stats).T
        there = across(here)
        top = jnp.maximum(here[0], there[0])
        tot = here[1] * jnp.exp(here[0] - top) + there[1] * jnp.exp(there[0] - top)
        logp = here[2] + there[2] - top - jnp.log(tot)
        return logp[None, :]

    return jax.shard_map(local_pass, mesh=mesh, in_specs=in_specs, out_specs=rows_spec, check_vma=False)
```

```python
import functools
import math
import jax
import jax.numpy as jnp
from jax import lax
from jax.experimental import pallas as pl
from jax.experimental.pallas import tpu as pltpu
from jax.sharding import PartitionSpec as P

RMS_EPS = 1e-6
ROPE_BASE = 10000.0
NEG_BIG = -1e30
LOG2E = 1.4426950408889634
CHUNKS = (2, 3, 3)
FF_BLOCK = 768
HEAD_BLOCK = 1024
KERNEL_MIB = 63
bf16, f32 = jnp.bfloat16, jnp.float32


def normed(x_in, gain):
    x_f = x_in.astype(f32)
    mean_sq = jnp.mean(x_f * x_f, axis=-1, keepdims=True)
    return (x_f * lax.rsqrt(mean_sq + RMS_EPS) * gain).astype(bf16)


def mm(a, b):
    return jnp.dot(a, b, preferred_element_type=f32)


def whole(shape):
    return pl.BlockSpec(shape, lambda *_: (0,) * len(shape), pipeline_mode=pl.Buffered(1))


ORDER_ONLY = pl.BlockSpec(memory_space=pl.ANY)


def call(body, flops, mib, grid, in_specs, out_shape, scratch, args, after):
    n_in, n_after = len(args), len(after)

    def run(*refs):
        body(*refs[:n_in], *refs[n_in + n_after:])

    return pl.pallas_call(
        run, grid=grid,
        in_specs=list(in_specs) + [ORDER_ONLY] * n_after,
        out_specs=[whole(o.shape) for o in out_shape], out_shape=out_shape, scratch_shapes=scratch,
        cost_estimate=pl.CostEstimate(flops=int(flops), bytes_accessed=0, transcendentals=0),
        compiler_params=pltpu.CompilerParams(vmem_limit_bytes=mib << 20),
    )(*args, *after)


def rotate(z, cos, sin):
    return (z * cos + pltpu.roll(z, z.shape[1] // 2, 1) * sin).astype(bf16)


def natural(i, rows):
    half, model = rows // 2, lax.axis_index('model')
    away = (1 - model) * half
    return i + jnp.where(i < half, away, -away)


def causal(rows):
    q = natural(lax.broadcasted_iota(jnp.int32, (rows, 1), 0), rows)
    k = natural(lax.broadcasted_iota(jnp.int32, (1, rows), 1), rows)
    return jnp.where(k <= q, 0.0, NEG_BIG)


def x_halves(xs, at, half):
    if at is not None:
        return [x[at:at + half] for x in xs]
    model = lax.axis_index('model')
    pick = lambda side: [x[pl.ds(pl.multiple_of(side * (x.shape[0] // 2), 16), x.shape[0] // 2)] for x in xs]
    return [jnp.concatenate(pick(side)) for side in (1 - model, model)]


def load_h(h, xs, at, gain):
    half = h.shape[0] // 2
    lo, hi = x_halves(xs, at, half)
    h[:half] = normed(lo, gain[...])
    h[half:] = normed(hi, gain[...])


def rope_rows(steps, base, first, rows):
    cos, sin = [], []
    sc, ss = steps[0, :rows // 2], steps[1, :rows // 2]
    for j in (first, first + 1):
        bc, bs = base[0, j:j + 1], base[1, j:j + 1]
        cos.append(bc * sc - bs * ss)
        sin.append(bs * sc + bc * ss)
    return jnp.concatenate(cos), jnp.concatenate(sin)


def layer_block(w, layer):
    return pl.BlockSpec((None,) + w.shape[1:], lambda *_: (layer,) + (0,) * (w.ndim - 1), pipeline_mode=pl.Buffered(1))


def rows_block(x, at, n):
    return pl.BlockSpec((pl.Element(n), pl.Element(x.shape[1])), lambda *_: (at, 0), pipeline_mode=pl.Buffered(1))


def prompt_body(parts, n_w, *refs):
    *xs, gain, steps, base = refs[:-3 * n_w - 2]
    ws, out, h = refs[-3 * n_w - 2:-2], refs[-2], refs[-1]
    load_h(h, xs, parts, gain)
    dim = ws[1].shape[1]
    cos, sin = rope_rows(steps, base, 0, h.shape[0])
    n_q = out.shape[1] // dim - 2 * n_w
    for i in range(0, n_q, 2):
        y = mm(h[...], jnp.concatenate([ws[0][i], ws[0][i + 1]], axis=1))
        out[:, i * dim:(i + 1) * dim] = rotate(y[:, :dim], cos, sin)
        out[:, (i + 1) * dim:(i + 2) * dim] = rotate(y[:, dim:], cos, sin)
    for i in range(n_w):
        y = mm(h[...], jnp.concatenate([ws[3 * i + 1][...], ws[3 * i + 2][...]], axis=1))
        c = (n_q + 2 * i) * dim
        out[:, c:c + dim] = rotate(y[:, :dim], cos, sin)
        out[:, c + dim:c + 2 * dim] = y[:, dim:].astype(bf16)


def prompt_qkv(xs, parts, rows, gain, ws, steps, base, with_q, after=()):
    n_heads, d_model, dim = ws[0][0][0].shape[1:]
    cols = (n_heads + 2 if with_q else 2 * len(ws)) * dim
    flat = [a for w in ws for a in w[0]]
    return call(functools.partial(prompt_body, parts, len(ws)), 4 * rows * d_model * cols, KERNEL_MIB, (1,),
                [whole(x.shape) for x in xs] + [whole(gain.shape), whole(steps.shape), whole(base.shape)] + [b for w in ws for b in w[1]],
                [jax.ShapeDtypeStruct((rows, cols), bf16)], [pltpu.VMEM((rows, d_model), bf16)],
                (*xs, gain, steps, base, *flat), after)[0]


def attend(q, kbuf, vbuf, bias):
    dim, keys, masked = q.shape[1], kbuf.shape[0], bias.shape[1]
    free = keys - masked
    s = lax.dot_general(q, kbuf[...], (((1,), (1,)), ((), ())), preferred_element_type=f32)
    diag = jnp.where(bias[...] < 0, NEG_BIG, s[:, free:])
    s = jnp.concatenate([s[:, :free], diag], axis=1) if free else diag
    top = jnp.max(s, axis=-1, keepdims=True)
    e = jnp.exp2((s - top) * (LOG2E / math.sqrt(dim)))
    p = (e * (1.0 / jnp.sum(e, axis=-1, keepdims=True))).astype(bf16)
    return mm(p, vbuf[...]).astype(bf16)


def attn_parts(n_x, n_w, parts, first, n_kv, n_seen, prompt, *refs):
    refs = list(refs)
    take = lambda n: [refs.pop(0) for _ in range(n)]
    xs = take(n_x)
    gain, steps, base = take(3)
    ws = [take(3) for _ in range(n_w)]
    pieces, seen = take(n_kv), take(n_seen)
    qkv_p = take(1)[0] if prompt else None
    out, kv_new, h, kbuf, vbuf, bias = take(6)
    bias_p = take(1)[0] if prompt else None
    rows, dim = h.shape[0], kbuf.shape[2]
    half, n_q = rows // 2, out.shape[1] // dim // n_w
    skip = qkv_p.shape[0] // 2 if prompt else 0

    def prepare():
        load_h(h, xs, parts, gain)
        bias[...] = causal(rows)
        if prompt:
            n_p, dev = qkv_p.shape[0], lax.axis_index('resp')
            bias_p[:, :n_p] = causal(n_p)
            for s in range(1, n_kv):
                bias_p[:, s * n_p:(s + 1) * n_p] = jnp.full((n_p, n_p), jnp.where(dev >= s, 0.0, NEG_BIG), f32)

    def side(m):
        wq, wk, wv = ws[m]
        cos, sin = rope_rows(steps, base, first, rows)
        fill, c = 0, 2 * m * dim
        for r in pieces + seen:
            n = r.shape[0]
            kbuf[m, fill:fill + n] = r[:, c:c + dim]
            vbuf[m, fill:fill + n] = r[:, c + dim:c + 2 * dim]
            fill += n
        y = mm(h[...], jnp.concatenate([wk[...], wv[...]], axis=1))
        k, v = rotate(y[:, :dim], cos, sin), y[:, dim:].astype(bf16)
        kv_new[:, c:c + dim], kv_new[:, c + dim:c + 2 * dim] = k, v
        kbuf[m, fill:], vbuf[m, fill:] = k, v
        if prompt:
            n_p = qkv_p.shape[0]
            for i in range(n_q):
                cols = slice(i * dim, (i + 1) * dim)
                mix = attend(qkv_p[:, cols], kbuf.at[m, :n_kv * n_p], vbuf.at[m, :n_kv * n_p], bias_p)
                out[:skip, cols] = mix[:skip]
                out[skip + half:2 * skip + half, cols] = mix[skip:]
        for i in range(0, n_q, 2):
            y = mm(h[...], jnp.concatenate([wq[i], wq[i + 1]], axis=1))
            for j in range(2):
                cols = slice((m * n_q + i + j) * dim, (m * n_q + i + j + 1) * dim)
                mix = attend(rotate(y[:, j * dim:(j + 1) * dim], cos, sin), kbuf.at[m], vbuf.at[m], bias)
                out[skip:skip + half, cols] = mix[:half]
                out[2 * skip + half:, cols] = mix[half:]

    def start():
        prepare()
        side(0)

    return [start] + [functools.partial(side, m) for m in range(1, n_w)]


def attn_body(*args):
    for part in attn_parts(*args):
        part()


def attn_chunk(xs, x_specs, parts, rows, gain, ws, steps, base, first, pieces, seen, qkv_p=None, after=()):
    d_model, dim = xs[0].shape[1], steps.shape[2]
    n_w, n_heads = len(ws), ws[0][2]
    keys = sum(a.shape[0] for a in pieces + seen) + rows
    n_p = qkv_p.shape[0] if qkv_p is not None else 0
    extra = [qkv_p] if n_p else []
    out = [jax.ShapeDtypeStruct((rows + n_p, n_w * n_heads * dim), bf16), jax.ShapeDtypeStruct((rows, 2 * n_w * dim), bf16)]
    buf = pltpu.VMEM((n_w, keys, dim), bf16)
    scratch = [pltpu.VMEM((rows, d_model), bf16), buf, buf, pltpu.VMEM((rows, rows), f32)]
    if n_p:
        scratch.append(pltpu.VMEM((n_p, n_p * len(pieces)), f32))
    rest = (*pieces, *seen, *extra)
    return call(functools.partial(attn_body, len(xs), n_w, parts, first, len(pieces), len(seen), bool(n_p)),
                n_w * (2 * rows * d_model * n_heads * dim + 8 * rows * keys * n_heads * dim), KERNEL_MIB, (1,),
                x_specs + [whole(gain.shape), whole(steps.shape), whole(base.shape)] + [b for w in ws for b in w[1]]
                + [whole(a.shape) for a in rest], out, scratch, (*xs, gain, steps, base, *[a for w in ws for a in w[0]], *rest), after)


def ffn_body(n_x, parts, layer, ff, attn, n_attn, *refs):
    refs = list(refs)
    take = lambda n: [refs.pop(0) for _ in range(n)]
    xs, gain, (wo_own, wo_far, wg, wu, wd), inputs = take(n_x), take(1)[0], take(5), take(n_attn)
    send, keep, xm = take(3)
    kv_new = take(1) if attn else []
    g, bo, bg, bu, bd, sems, *spare = refs
    step, blk, half = pl.program_id(0), bg.shape[2], send.shape[0]
    n_blk = pl.cdiv(ff, blk)
    rest = ff - (n_blk - 1) * blk
    n_pre = 1 + (attn[0] if attn else 0)

    def block_copies(j, slot, n):
        at = pl.multiple_of(j * blk, 128)
        return [pltpu.make_async_copy(wg.at[layer, :, pl.ds(at, n)], bg.at[slot, :, :n], sems.at[2 + 3 * slot]),
                pltpu.make_async_copy(wu.at[layer, :, pl.ds(at, n)], bu.at[slot, :, :n], sems.at[3 + 3 * slot]),
                pltpu.make_async_copy(wd.at[layer, pl.ds(at, n)], bd.at[slot, :n], sems.at[4 + 3 * slot])]

    @pl.when(step == 0)
    def _():
        wo_copies = [pltpu.make_async_copy(wo_own.at[layer], bo.at[0], sems.at[0]), pltpu.make_async_copy(wo_far, bo.at[1], sems.at[1])]
        for copy in wo_copies + block_copies(0, 0, blk):
            copy.start()

    if attn:
        mix, *buffers = spare
        for at, piece in enumerate(attn_parts(n_x, *attn, *xs, *inputs, mix, *kv_new, g, *buffers)):
            pl.when(step == at)(piece)

    @pl.when(step == n_pre - 1)
    def _():
        if attn:
            own, far = mix[:, :bo.shape[1]], mix[:, bo.shape[1]:]
        elif n_attn > 1:
            own, far = inputs[0][...], jnp.concatenate([inputs[1][half:], inputs[1][:half]])
        else:
            own, far = inputs[0][:, :bo.shape[1]], inputs[0][:, bo.shape[1]:]
        lo, hi = x_halves(xs, parts, half)
        wo_copies = [pltpu.make_async_copy(wo_own.at[layer], bo.at[0], sems.at[0]), pltpu.make_async_copy(wo_far, bo.at[1], sems.at[1])]
        wo_copies[0].wait()
        acc = mm(own, bo[0])
        wo_copies[1].wait()
        acc += mm(far, bo[1])
        g[:half] = normed((lo.astype(f32) + acc[:half]).astype(bf16), gain[...])
        mid = (hi.astype(f32) + acc[half:]).astype(bf16)
        xm[...] = mid
        g[half:] = normed(mid, gain[...])
        send[...] = jnp.zeros_like(send)
        keep[...] = jnp.zeros_like(keep)

    def part(slot, n):
        gate, up = mm(g[...], bg[slot, :, :n]), mm(g[...], bu[slot, :, :n])
        u = (gate * (1.0 / (1.0 + jnp.exp(-gate))) * up).astype(bf16)
        d = mm(u, bd[slot, :n])
        send[...] += d[:half]
        keep[...] += d[half:]

    j = step - n_pre
    slot = lax.rem(step + n_pre, 2)

    @pl.when((j >= 0) & (j + 1 < n_blk - 1))
    def _():
        for copy in block_copies(j + 1, 1 - slot, blk):
            copy.start()

    @pl.when(j + 1 == n_blk - 1)
    def _():
        for copy in block_copies(n_blk - 1, (n_blk - 1) % 2, rest):
            copy.start()

    @pl.when((j >= 0) & (j < n_blk - 1))
    def _():
        for copy in block_copies(j, slot, blk):
            copy.wait()
        part(slot, blk)

    @pl.when(j == n_blk - 1)
    def _():
        for copy in block_copies(n_blk - 1, (n_blk - 1) % 2, rest):
            copy.wait()
        part((n_blk - 1) % 2, rest)


def ffn_chunk(xs, x_specs, parts, layer, gain, wo_own, wo_far, wg, wu, wd, mix=None, attn=None, after=()):
    d_model, ff, blk = xs[0].shape[1], wg.shape[2], FF_BLOCK
    width = wo_far.shape[0]
    big = [pl.BlockSpec(memory_space=pl.ANY)] * 5
    flops = 6
    if attn is None:
        rows, inputs, in_specs, attn_static, spare, more = mix[0].shape[0], list(mix), [whole(a.shape) for a in mix], None, [], []
    else:
        rows, gain_a, ws, steps, base, first, pieces, seen = attn
        dim = steps.shape[2]
        keys = sum(a.shape[0] for a in pieces + seen) + rows
        inputs = [gain_a, steps, base, *[a for w in ws for a in w[0]], *pieces, *seen]
        in_specs = [whole(a.shape) for a in (gain_a, steps, base)] + [b for w in ws for b in w[1]] + [whole(a.shape) for a in pieces + seen]
        attn_static = (len(ws), parts, first, len(pieces), len(seen), False)
        buf = pltpu.VMEM((len(ws), keys, dim), bf16)
        spare = [pltpu.VMEM((rows, len(ws) * width), bf16), buf, buf, pltpu.VMEM((rows, rows), f32)]
        more = [jax.ShapeDtypeStruct((rows, 2 * len(ws) * dim), bf16)]
        flops = 8
    half = rows // 2
    out = [jax.ShapeDtypeStruct((half, d_model), f32)] * 2 + [jax.ShapeDtypeStruct((half, d_model), bf16)] + more
    scratch = [pltpu.VMEM((rows, d_model), bf16), pltpu.VMEM((2, width, d_model), bf16), pltpu.VMEM((2, d_model, blk), bf16),
               pltpu.VMEM((2, d_model, blk), bf16), pltpu.VMEM((2, blk, d_model), bf16), pltpu.SemaphoreType.DMA((8,))] + spare
    return call(functools.partial(ffn_body, len(xs), parts, layer, ff, attn_static, len(inputs)),
                flops * rows * d_model * ff, KERNEL_MIB, (1 + (attn_static[0] if attn else 0) + pl.cdiv(ff, blk),),
                x_specs + [whole(gain.shape)] + big + in_specs, out, scratch,
                (*xs, gain, wo_own, wo_far, wg, wu, wd, *inputs), after)


def head_body(row, xa, xb, gain, w, tgt, out, h, logits, top, pick):
    step, blk = pl.program_id(0), w.shape[1]

    @pl.when(step == 0)
    def _():
        load_h(h, (xa, xb), 0, gain)
        top[...] = jnp.full_like(top, NEG_BIG)
        pick[...] = jnp.zeros_like(pick)

    s = mm(h[...], w[...])
    logits[step] = s
    lanes = top.shape[1]
    hit = tgt[row:row + top.shape[0]] - step * blk
    lane = lax.broadcasted_iota(jnp.int32, top.shape, 1)
    best, found = top[...], pick[...]
    for c in range(0, blk, lanes):
        piece = s[:, c:c + lanes]
        best = jnp.maximum(best, piece)
        found += jnp.where(lane + c == hit, piece, 0.0)
    top[...], pick[...] = best, found

    @pl.when(step == pl.num_programs(0) - 1)
    def _():
        peak = jnp.max(top[...], axis=-1, keepdims=True)
        tot = jnp.zeros_like(top)
        for b in range(logits.shape[0]):
            for c in range(0, blk, lanes):
                tot += jnp.exp(logits[b, :, c:c + lanes] - peak)
        tot = jnp.sum(tot, axis=-1, keepdims=True)
        hits = jnp.sum(pick[...], axis=-1, keepdims=True)
        out[...] = jnp.where(lane == 0, peak, jnp.where(lane == 1, tot, hits))


def head_chunk(xa, xb, gain, w, tgt, row, after=()):
    d_model, vocab, blk = xa.shape[1], w.shape[1], HEAD_BLOCK
    rows = 2 * xa.shape[0]
    side = pltpu.VMEM((rows, 128), f32)
    return call(functools.partial(head_body, row), 4 * rows * d_model * vocab, KERNEL_MIB, (vocab // blk,),
                [whole(xa.shape), whole(xb.shape), whole(gain.shape), pl.BlockSpec((d_model, blk), lambda j: (0, j)), whole(tgt.shape)],
                [jax.ShapeDtypeStruct((rows, 128), f32)],
                [pltpu.VMEM((rows, d_model), bf16), pltpu.VMEM((vocab // blk, rows, blk), f32), side, side],
                (xa, xb, gain, w, tgt), after)[0]


def rope_tables(positions, head_dim):
    inv_freq = jnp.exp(jnp.arange(0, head_dim, 2, dtype=f32) * (-math.log(ROPE_BASE) / head_dim))
    angles = positions.astype(f32)[:, None] * inv_freq[None, :]
    cos, sin = jnp.cos(angles), jnp.sin(angles)
    return jnp.stack([jnp.concatenate([cos, cos], axis=1), jnp.concatenate([-sin, sin], axis=1)])


def held(x, *after):
    return lax.optimization_barrier((x, *after))[0]


def solution(mesh):
    group = mesh.shape['resp']
    rows_spec = P(('prompts', 'resp'), None)
    in_specs = (rows_spec, P(('prompts', 'resp'), None, None), rows_spec, P(), P(),
                P(None, None, 'model', None), P(None, None, 'model', None), P(None, None, 'model', None),
                P(None, 'model', None, None), P(None, None, 'model'), P(None, None, 'model'),
                P(None, 'model', None), P(), P(None, 'model'))

    def across(x):
        return lax.ppermute(x, 'model', [(0, 1), (1, 0)])

    def all_pieces(x):
        return [x] + [lax.ppermute(x, 'resp', [(i, (i + s) % group) for i in range(group)]) for s in range(1, group)]

    def local_pass(x_piece, x_own, tgt_own, attn_norm, mlp_norm, w_q, w_k, w_v, w_o, w_gate, w_up, w_down, final_norm, w_head):
        n_layers, d_model, heads_loc, dim = w_q.shape
        piece_len, resp_len = x_piece.shape[0], x_own.shape[1]
        prompt_len = piece_len * group
        dev_idx, model_idx = lax.axis_index('resp'), lax.axis_index('model')
        sizes = [resp_len * n // sum(CHUNKS) for n in CHUNKS]
        starts = [sum(sizes[:c]) for c in range(len(sizes))]
        n_chunks = len(sizes)

        def joined(part):
            return lax.all_gather(part, 'resp', axis=0, tiled=True)

        w_out = w_o.reshape(n_layers, heads_loc * dim, d_model)
        part = heads_loc * dim // group

        def wo_part(l, *after):
            x = lax.dynamic_slice(w_out, (l, dev_idx * part, 0), (1, part, d_model))[0]
            return across(held(x, *after))

        def own_heads(l, *after):
            w = (held(w_q, *after)[l].transpose(1, 0, 2)[None], w_k[l].reshape(1, d_model, dim), w_v[l].reshape(1, d_model, dim))
            return w, [layer_block(a, 0) for a in w], heads_loc

        def far_heads(w):
            spec = lambda n, i: pl.BlockSpec((n, d_model, dim), lambda *_: (i, 0, 0), pipeline_mode=pl.Buffered(1))
            return (w, w, w), [spec(heads_loc, 0), spec(None, heads_loc), spec(None, heads_loc + 1)], heads_loc

        def halves(x, at, n):
            half = n // 2
            return (lax.dynamic_slice_in_dim(x, at + (1 - model_idx) * half, half, 0),
                    lax.dynamic_slice_in_dim(x, at + model_idx * half, half, 0))

        steps = rope_tables(jnp.arange(max(sizes) // 2), dim)
        both = jnp.stack([1 - model_idx, model_idx])
        base = rope_tables(jnp.concatenate([dev_idx * piece_len + both * (piece_len // 2)] + [
            prompt_len + at + both * (n // 2) for at, n in zip(starts, sizes)]), dim)
        x_rows = x_own[0]

        def source(l, c, with_prompt):
            if l == 0:
                xs = ([x_piece] if with_prompt else []) + [x_rows]
                return xs, ([whole(x_piece.shape)] if with_prompt else []) + [rows_block(x_rows, starts[c], sizes[c])], None
            return x_r[c], [whole(x.shape) for x in x_r[c]], 0 if c else piece_len // 2

        x_r, far = {}, {}
        pending = {}

        def mlp_of(l, c, wo_far, after, mix=None, attn=None):
            xs, specs, parts = source(l, c, c == 0)
            *pending[c], = ffn_chunk(xs, specs, parts, l, mlp_norm[l][None], w_out, wo_far, w_gate, w_up, w_down, mix, attn, after)
            return pending[c][1]

        def send(c, *after):
            far[c] = across(held(pending[c][0], *after))

        def collect(c, *after):
            _, keep, xm = pending.pop(c)[:3]
            mine = (xm.astype(f32) + (keep + held(far.pop(c), *after))).astype(bf16)
            x_r[c] = [across(mine), mine]
            return mine

        end = n_chunks - 1
        gain = attn_norm[0][None]
        w_own = own_heads(0)
        qkv_p = prompt_qkv([x_piece], None, piece_len, gain, [w_own], steps, base, True)
        pieces = all_pieces(qkv_p[:, heads_loc * dim:])
        wo_sent = [wo_part(0, qkv_p)]
        w_next = own_heads(1, qkv_p)
        heads = jnp.concatenate([w_next[0][0][0], w_next[0][1], w_next[0][2]])
        per = heads.shape[0] // group
        w_part = across(lax.dynamic_slice_in_dim(heads, dev_idx * per, per, 0))
        a, seen, tail = [], [], ()
        for c in range(n_chunks):
            xs, specs, parts = source(0, c, False)
            mix, kv = attn_chunk(xs, specs, parts, sizes[c], gain, [w_own], steps, base, 2 + 2 * c, pieces, list(seen),
                                 qkv_p if c == 0 else None, tail)
            seen.append(kv)
            a.append((mix, across(mix)))
            tail = (mix,)
            if c == 0:
                wo_far = [joined(held(wo_sent[0], mix))]
        wo_sent.append(wo_part(1, a[-1][0]))
        for c in range(n_chunks):
            tail = (mlp_of(0, c, wo_far[0], tail, mix=a[c]),)
            if c == 0:
                w_far = far_heads(joined(held(w_part, *tail)))
                send(c)
            elif c < end or c == 1:
                tail = (*tail, collect(c - 1, *tail))
                if c < end:
                    send(c)
            if c == 1:
                tgt = tgt_own[0] - model_idx * w_head.shape[1]
                tgt = held(jnp.concatenate([h for at, n in zip(starts, sizes) for h in halves(tgt, at, n)]), *tail)[:, None]
                wo_far.append(joined(held(wo_sent[1], *tail)))
        gain = attn_norm[1][None]
        both_w = [w_next, w_far]
        kv_p = prompt_qkv(x_r[0], 0, piece_len, gain, both_w, steps, base, False, tail)
        pieces = all_pieces(kv_p)
        tail = (kv_p, collect(end - 1, kv_p)) if end > 1 else (kv_p,)
        send(end)
        seen = []
        tail = (mlp_of(1, 0, wo_far[1], tail, attn=(sizes[0], gain, both_w, steps, base, 2, pieces, [])),)
        seen.append(pending[0][3])
        tail = (*tail, collect(end, *tail))
        send(0)

        def attention(c, ws, after):
            xs, specs, parts = source(1, c, False)
            mix, kv = attn_chunk(xs, specs, parts, sizes[c], gain, ws, steps, base, 2 + 2 * c, pieces, list(seen), None, after)
            seen.append(kv)
            return mix

        mixes = {}
        for c in range(1, n_chunks):
            mix = attention(c, both_w[:1], tail)
            mixes[c] = [mix, across(mix)]
            tail = (mix,)
        for c in range(1, n_chunks):
            tail = (mlp_of(1, c, wo_far[1], tail, mix=mixes[c]),)
            send(c)
        for c in range(n_chunks):
            tail = (*tail, collect(c, *tail))
        stats = []
        for c in range(n_chunks):
            out = head_chunk(*x_r[c], final_norm[None], w_head, tgt, starts[c], tail)
            tail = (out,)
            stats.append(jnp.concatenate(halves(out[:, :3], 0, sizes[c])))
        here = jnp.concatenate(stats).T
        there = across(here)
        top = jnp.maximum(here[0], there[0])
        tot = here[1] * jnp.exp(here[0] - top) + there[1] * jnp.exp(there[0] - top)
        logp = here[2] + there[2] - top - jnp.log(tot)
        return logp[None, :]

    return jax.shard_map(local_pass, mesh=mesh, in_specs=in_specs, out_specs=rows_spec, check_vma=False)
```
